8 devices in a mesh: model: 4 (over z, y, x), data: 2 (over core).
Axes of the slice: x: 2, y: 2, z: 1, core: 2. Of those that a mesh axis runs over, the one named last changes fastest.
Arguments:
- x_tokens: bfloat16 [8192, 3072], P('data')
- dy_tokens: bfloat16 [8192, 3072], P('data')
- w_col: bfloat16 [2, 3072, 3072], P(None, None, 'model')
- w_row: bfloat16 [2, 3072, 3072], P(None, 'model')
- a_old_col: float32 [2, 3072, 3072], replicated
- s_old_col: float32 [2, 3072, 768], P(None, 'model')
- a_old_row: float32 [2, 3072, 768], P(None, 'model')
- s_old_row: float32 [2, 3072, 3072], replicated
- a_inv_col: float32 [2, 3072, 3072], replicated
- s_inv_col: float32 [2, 3072, 768], P(None, 'model')
- a_inv_row: float32 [2, 3072, 768], P(None, 'model')
- s_inv_row: float32 [2, 3072, 3072], replicated
Outputs:
- output 1: float32 [2, 3072, 3072], P(None, None, 'model')
- output 2: float32 [2, 3072, 3072], P(None, 'model')
- output 3: float32 [2, 3072, 3072], replicated
- output 4: float32 [2, 3072, 768], P(None, 'model')
- output 5: float32 [2, 3072, 768], P(None, 'model')
- output 6: float32 [2, 3072, 3072], replicated
All inputs are finite; a program needn't handle non-finite values.
Results may differ from the reference program's by a relative error of at most 0.00613152.
Values are sent between devices in bfloat16 or wider.
A program may use at most 2.25 GiB of HBM per device.

```python
import math
import jax
import jax.numpy as jnp
from jax import lax

HIDDEN = 3072
TOKENS_DEV = 4096
DATA_WAYS = 2
MODEL_WAYS = 4
BATCH_ROWS = TOKENS_DEV * DATA_WAYS
BLOCK_DIM = HIDDEN // MODEL_WAYS
FACTOR_DECAY = 0.8
GELU_SCALE = math.sqrt(2.0 / math.pi)
GELU_CUBIC = 0.044715
EXACT = lax.Precision.HIGHEST


def gelu_value(pre_act):
    tanh_arg = GELU_SCALE * (pre_act + GELU_CUBIC * pre_act * pre_act * pre_act)
    return 0.5 * pre_act * (1.0 + jnp.tanh(tanh_arg))


def gelu_slope(pre_act):
    tanh_arg = GELU_SCALE * (pre_act + GELU_CUBIC * pre_act * pre_act * pre_act)
    tanh_val = jnp.tanh(tanh_arg)
    return 0.5 * (1.0 + tanh_val) + 0.5 * pre_act * (1.0 - tanh_val * tanh_val) * GELU_SCALE * (1.0 + 3.0 * GELU_CUBIC * pre_act * pre_act)


def activate(pre_act):
    return gelu_value(pre_act.astype(jnp.float32)).astype(jnp.bfloat16)


def back_gate(grad_act, pre_act):
    return (grad_act.astype(jnp.float32) * gelu_slope(pre_act.astype(jnp.float32))).astype(jnp.bfloat16)


def sym_draw(rand_key, lead_count, mat_dim, spread):
    diag_key, noise_key = jax.random.split(rand_key)
    diag_vals = jax.random.uniform(diag_key, (lead_count, mat_dim), jnp.float32, 0.5, 1.5)
    sym_noise = jax.random.normal(noise_key, (lead_count, mat_dim, mat_dim), jnp.float32)
    sym_noise = (sym_noise + jnp.swapaxes(sym_noise, 1, 2)) * (spread / math.sqrt(2.0 * mat_dim))
    return sym_noise + diag_vals[:, :, None] * jnp.eye(mat_dim, dtype=jnp.float32)


def block_draw(rand_key, spread):
    return sym_draw(rand_key, 2 * MODEL_WAYS, BLOCK_DIM, spread).reshape(2, HIDDEN, BLOCK_DIM)


def token_draw(rand_key):
    mean_key, scale_key, base_key = jax.random.split(rand_key, 3)
    shard_mean = jax.random.normal(mean_key, (DATA_WAYS, 1, HIDDEN), jnp.float32) * (0.5 * HIDDEN ** -0.25)
    shard_scale = jnp.exp2(jax.random.uniform(scale_key, (DATA_WAYS, 1, 1), jnp.float32, -1.0, 1.0))
    base_vals = jax.random.normal(base_key, (DATA_WAYS, TOKENS_DEV, HIDDEN), jnp.float32)
    return (base_vals * shard_scale + shard_mean).reshape(BATCH_ROWS, HIDDEN).astype(jnp.bfloat16)


def setup_inputs(seed: int = 0) -> dict:
    key_list = jax.random.split(jax.random.key(seed), 12)
    weight_scale = HIDDEN ** -0.5
    return {
        'x_tokens': token_draw(key_list[0]),
        'dy_tokens': token_draw(key_list[1]),
        'w_col': (jax.random.normal(key_list[2], (2, HIDDEN, HIDDEN), jnp.float32) * weight_scale).astype(jnp.bfloat16),
        'w_row': (jax.random.normal(key_list[3], (2, HIDDEN, HIDDEN), jnp.float32) * weight_scale).astype(jnp.bfloat16),
        'a_old_col': sym_draw(key_list[4], 2, HIDDEN, 0.3),
        's_old_col': block_draw(key_list[5], 0.3),
        'a_old_row': block_draw(key_list[6], 0.3),
        's_old_row': sym_draw(key_list[7], 2, HIDDEN, 0.3),
        'a_inv_col': sym_draw(key_list[8], 2, HIDDEN, 0.2),
        's_inv_col': block_draw(key_list[9], 0.2),
        'a_inv_row': block_draw(key_list[10], 0.2),
        's_inv_row': sym_draw(key_list[11], 2, HIDDEN, 0.2),
    }


def gram_mat(left_mat, right_mat):
    return jnp.dot(left_mat.T, right_mat, preferred_element_type=jnp.float32) / BATCH_ROWS


def block_gram(left_mat, right_mat):
    left_blocks = jnp.swapaxes(left_mat.reshape(BATCH_ROWS, MODEL_WAYS, BLOCK_DIM), 0, 1)
    right_blocks = jnp.swapaxes(right_mat.reshape(BATCH_ROWS, MODEL_WAYS, BLOCK_DIM), 0, 1)
    blocks = lax.map(lambda block_pair: jnp.dot(block_pair[0].T, block_pair[1], preferred_element_type=jnp.float32), (left_blocks, right_blocks))
    return blocks.reshape(HIDDEN, BLOCK_DIM) / BATCH_ROWS


def precondition_col(a_inv, grad_mat, s_inv_blocks):
    left_done = jnp.dot(a_inv, grad_mat, precision=EXACT).reshape(HIDDEN, MODEL_WAYS, BLOCK_DIM)
    right_blocks = s_inv_blocks.reshape(MODEL_WAYS, BLOCK_DIM, BLOCK_DIM)
    return jnp.einsum('dmi,mij->dmj', left_done, right_blocks, precision=EXACT).reshape(HIDDEN, HIDDEN)


def precondition_row(a_inv_blocks, grad_mat, s_inv):
    left_blocks = a_inv_blocks.reshape(MODEL_WAYS, BLOCK_DIM, BLOCK_DIM)
    left_done = jnp.einsum('mij,mjk->mik', left_blocks, grad_mat.reshape(MODEL_WAYS, BLOCK_DIM, HIDDEN), precision=EXACT).reshape(HIDDEN, HIDDEN)
    return jnp.dot(left_done, s_inv, precision=EXACT)


def blend_factor(old_mats, first_new, second_new):
    return FACTOR_DECAY * old_mats + (1.0 - FACTOR_DECAY) * jnp.stack([first_new, second_new])


def reference(x_tokens, dy_tokens, w_col, w_row, a_old_col, s_old_col, a_old_row, s_old_row, a_inv_col, s_inv_col, a_inv_row, s_inv_row):
    z_one = jnp.dot(x_tokens, w_col[0], preferred_element_type=jnp.float32).astype(jnp.bfloat16)
    h_one = activate(z_one)
    z_two = jnp.dot(h_one, w_row[0], preferred_element_type=jnp.float32).astype(jnp.bfloat16)
    h_two = activate(z_two)
    z_three = jnp.dot(h_two, w_col[1], preferred_element_type=jnp.float32).astype(jnp.bfloat16)
    h_three = activate(z_three)
    g_three = back_gate(jnp.dot(dy_tokens, w_row[1].T, preferred_element_type=jnp.float32).astype(jnp.bfloat16), z_three)
    g_two = back_gate(jnp.dot(g_three, w_col[1].T, preferred_element_type=jnp.float32).astype(jnp.bfloat16), z_two)
    g_one = back_gate(jnp.dot(g_two, w_row[0].T, preferred_element_type=jnp.float32).astype(jnp.bfloat16), z_one)
    u_col = jnp.stack([
        precondition_col(a_inv_col[0], gram_mat(x_tokens, g_one), s_inv_col[0]),
        precondition_col(a_inv_col[1], gram_mat(h_two, g_three), s_inv_col[1]),
    ])
    u_row = jnp.stack([
        precondition_row(a_inv_row[0], gram_mat(h_one, g_two), s_inv_row[0]),
        precondition_row(a_inv_row[1], gram_mat(h_three, dy_tokens), s_inv_row[1]),
    ])
    a_new_col = blend_factor(a_old_col, gram_mat(x_tokens, x_tokens), gram_mat(h_two, h_two))
    s_new_col = blend_factor(s_old_col, block_gram(g_one, g_one), block_gram(g_three, g_three))
    a_new_row = blend_factor(a_old_row, block_gram(h_one, h_one), block_gram(h_three, h_three))
    s_new_row = blend_factor(s_old_row, gram_mat(g_two, g_two), gram_mat(dy_tokens, dy_tokens))
    return (u_col, u_row, a_new_col, s_new_col, a_new_row, s_new_row)
```

```python
import math
import jax
import jax.numpy as jnp
from jax import lax
from jax.sharding import PartitionSpec as P

FACTOR_DECAY = 0.8
GELU_SCALE = math.sqrt(2.0 / math.pi)
GELU_CUBIC = 0.044715
EXACT = lax.Precision.HIGHEST
TN_DIMS = (((0,), (0,)), ((), ()))
NT_DIMS = (((1,), (1,)), ((), ()))


def gelu_value(pre_act):
    tanh_arg = GELU_SCALE * (pre_act + GELU_CUBIC * pre_act * pre_act * pre_act)
    return 0.5 * pre_act * (1.0 + jnp.tanh(tanh_arg))


def gelu_slope(pre_act):
    tanh_arg = GELU_SCALE * (pre_act + GELU_CUBIC * pre_act * pre_act * pre_act)
    tanh_val = jnp.tanh(tanh_arg)
    return 0.5 * (1.0 + tanh_val) + 0.5 * pre_act * (1.0 - tanh_val * tanh_val) * GELU_SCALE * (1.0 + 3.0 * GELU_CUBIC * pre_act * pre_act)


def activate(pre_act):
    return gelu_value(pre_act.astype(jnp.float32)).astype(jnp.bfloat16)


def back_gate(grad_act, pre_act):
    return (grad_act.astype(jnp.float32) * gelu_slope(pre_act.astype(jnp.float32))).astype(jnp.bfloat16)


def matmul(left_mat, right_mat):
    return jnp.dot(left_mat, right_mat, preferred_element_type=jnp.float32)


def matmul_tn(left_mat, right_mat):
    return lax.dot_general(left_mat, right_mat, TN_DIMS, preferred_element_type=jnp.float32)


def matmul_nt(left_mat, right_mat):
    return lax.dot_general(left_mat, right_mat, NT_DIMS, preferred_element_type=jnp.float32)


def exact_dot(left_mat, right_mat):
    return jnp.dot(left_mat, right_mat, precision=EXACT, preferred_element_type=jnp.float32)


def blend_factor(old_mats, first_new, second_new, inv_rows):
    return FACTOR_DECAY * old_mats + (1.0 - FACTOR_DECAY) * inv_rows * jnp.stack([first_new, second_new])


def solution(mesh):
    data_ways = mesh.shape['data']
    model_ways = mesh.shape['model']

    def to_rows(col_part):
        return lax.all_to_all(col_part, 'model', split_axis=0, concat_axis=1, tiled=True)

    def gather_weight(part):
        half = part.shape[0] // data_ways
        mine = lax.dynamic_slice_in_dim(part, lax.axis_index('data') * half, half, 0)
        return lax.all_gather(mine, ('model', 'data'), axis=0, tiled=True)

    def precondition_col(a_inv, grad_half, s_inv):
        half_rows = grad_half.shape[0]
        right_done = lax.all_gather(exact_dot(grad_half, s_inv), 'data', axis=0, tiled=True)
        a_rows = lax.dynamic_slice_in_dim(a_inv, lax.axis_index('data') * half_rows, half_rows, 0)
        return lax.all_gather(exact_dot(a_rows, right_done), 'data', axis=0, tiled=True)

    def precondition_row(a_inv, grad_half, s_inv):
        half_cols = grad_half.shape[1]
        left_done = lax.all_gather(exact_dot(a_inv, grad_half), 'data', axis=1, tiled=True)
        s_cols = lax.dynamic_slice_in_dim(s_inv, lax.axis_index('data') * half_cols, half_cols, 1)
        return lax.all_gather(exact_dot(left_done, s_cols), 'data', axis=1, tiled=True)

    def shard_body(x_tokens, dy_tokens, w_col, w_row, a_old_col, s_old_col, a_old_row, s_old_row, a_inv_col, s_inv_col, a_inv_row, s_inv_row):
        inv_rows = 1.0 / (x_tokens.shape[0] * data_ways)
        w_two = gather_weight(w_row[0])
        w_three_t = gather_weight(w_col[1].T)
        z_one = matmul(x_tokens, w_col[0]).astype(jnp.bfloat16)
        h_one = activate(z_one)
        dh_three = matmul_nt(dy_tokens, w_row[1]).astype(jnp.bfloat16)
        h_one_t = to_rows(h_one)
        dh_three_t = to_rows(dh_three)
        z_two_t = matmul(h_one_t, w_two).astype(jnp.bfloat16)
        h_two_t = activate(z_two_t)
        h_two = lax.all_gather(h_two_t, 'model', axis=0, tiled=True)
        a_one = matmul_tn(x_tokens, x_tokens)
        a_two = matmul_tn(h_one, h_one)
        z_three_t = matmul_nt(h_two_t, w_three_t).astype(jnp.bfloat16)
        g_three_t = back_gate(dh_three_t, z_three_t)
        dh_two_t = matmul(g_three_t, w_three_t).astype(jnp.bfloat16)
        g_two_t = back_gate(dh_two_t, z_two_t)
        g_two = lax.all_gather(g_two_t, 'model', axis=0, tiled=True)


        h_two, a_one, a_two, g_two_t = lax.optimization_barrier((h_two, a_one, a_two, g_two_t))
        z_three = matmul(h_two, w_col[1]).astype(jnp.bfloat16)
        h_three = activate(z_three)
        g_three = back_gate(dh_three, z_three)
        grad_four = matmul_tn(h_three, dy_tokens)
        grad_three = matmul_tn(h_two, g_three)
        a_three = matmul_tn(h_two, h_two)
        a_four = matmul_tn(h_three, h_three)
        s_three = matmul_tn(g_three, g_three)
        s_four = matmul_tn(dy_tokens, dy_tokens)
        g_two, grad_three, grad_four, a_one, a_two, a_three, a_four, s_three, s_four = lax.optimization_barrier(
            (g_two, grad_three, grad_four, a_one, a_two, a_three, a_four, s_three, s_four))
        grad_four = lax.psum_scatter(grad_four, 'data', scatter_dimension=1, tiled=True) * inv_rows
        grad_three = lax.psum_scatter(grad_three, 'data', scatter_dimension=0, tiled=True) * inv_rows

        g_one = back_gate(matmul_nt(g_two, w_row[0]).astype(jnp.bfloat16), z_one)
        grad_one = lax.psum_scatter(matmul_tn(x_tokens, g_one), 'data', scatter_dimension=0, tiled=True) * inv_rows
        grad_two = lax.psum_scatter(matmul_tn(h_one, g_two), 'data', scatter_dimension=1, tiled=True) * inv_rows
        s_two = matmul_tn(g_two, g_two)
        s_one = matmul_tn(g_one, g_one)
        a_one, a_two, a_three, a_four, s_three, s_four = lax.psum([a_one, a_two, a_three, a_four, s_three, s_four], 'data')
        s_one, s_two, a_one, a_two, a_three, a_four, s_three, s_four = lax.optimization_barrier(
            (s_one, s_two, a_one, a_two, a_three, a_four, s_three, s_four))
        s_one, s_two = lax.psum([s_one, s_two], 'data')

        u_col = jnp.stack([precondition_col(a_inv_col[0], grad_one, s_inv_col[0]), precondition_col(a_inv_col[1], grad_three, s_inv_col[1])])
        u_row = jnp.stack([precondition_row(a_inv_row[0], grad_two, s_inv_row[0]), precondition_row(a_inv_row[1], grad_four, s_inv_row[1])])
        a_new_col = blend_factor(a_old_col, a_one, a_three, inv_rows)
        s_new_col = blend_factor(s_old_col, s_one, s_three, inv_rows)
        a_new_row = blend_factor(a_old_row, a_two, a_four, inv_rows)
        s_new_row = blend_factor(s_old_row, s_two, s_four, inv_rows)
        return (u_col, u_row, a_new_col, s_new_col, a_new_row, s_new_row)

    batch_split = P('data', None)
    col_split = P(None, None, 'model')
    row_split = P(None, 'model', None)
    replicated = P()
    return jax.shard_map(
        shard_body,
        mesh=mesh,
        in_specs=(batch_split, batch_split, col_split, row_split, replicated, row_split, row_split, replicated, replicated, row_split, row_split, replicated),
        out_specs=(col_split, row_split, replicated, row_split, row_split, replicated),
        check_vma=False,
    )
```

```python
import functools
import math
import jax
import jax.numpy as jnp
from jax import lax
from jax.experimental import pallas as pl
from jax.experimental.pallas import tpu as pltpu
from jax.sharding import PartitionSpec as P

FACTOR_DECAY = 0.8
GELU_SCALE = math.sqrt(2.0 / math.pi)
GELU_CUBIC = 0.044715
EXACT = lax.Precision.HIGHEST
TN_DIMS = (((0,), (0,)), ((), ()))
NT_DIMS = (((1,), (1,)), ((), ()))


def gelu_value(pre_act):
    tanh_arg = GELU_SCALE * (pre_act + GELU_CUBIC * pre_act * pre_act * pre_act)
    return 0.5 * pre_act * (1.0 + jnp.tanh(tanh_arg))


def gelu_slope(pre_act):
    tanh_arg = GELU_SCALE * (pre_act + GELU_CUBIC * pre_act * pre_act * pre_act)
    tanh_val = jnp.tanh(tanh_arg)
    return 0.5 * (1.0 + tanh_val) + 0.5 * pre_act * (1.0 - tanh_val * tanh_val) * GELU_SCALE * (1.0 + 3.0 * GELU_CUBIC * pre_act * pre_act)


def activate(pre_act):
    return gelu_value(pre_act.astype(jnp.float32)).astype(jnp.bfloat16)


def back_gate(grad_act, pre_act):
    return (grad_act.astype(jnp.float32) * gelu_slope(pre_act.astype(jnp.float32))).astype(jnp.bfloat16)


def matmul(left_mat, right_mat):
    return jnp.dot(left_mat, right_mat, preferred_element_type=jnp.float32)


def matmul_tn(left_mat, right_mat):
    return lax.dot_general(left_mat, right_mat, TN_DIMS, preferred_element_type=jnp.float32)


def matmul_nt(left_mat, right_mat):
    return lax.dot_general(left_mat, right_mat, NT_DIMS, preferred_element_type=jnp.float32)


def exact_dot(left_mat, right_mat):
    return jnp.dot(left_mat, right_mat, precision=EXACT, preferred_element_type=jnp.float32)


SWAP = [(0, 1), (1, 0)]
BLEND_ROWS = 256


def blend_blocks(old_mats, first_pair, second_pair, inv_rows):
    return FACTOR_DECAY * old_mats + (1.0 - FACTOR_DECAY) * inv_rows * jnp.stack([sum(first_pair), sum(second_pair)])


def blend_kernel(term_count, scale, old_ref, *refs):
    total = refs[0][...]
    for term in range(1, term_count):
        total = total + refs[term][...]
    refs[-1][0] = FACTOR_DECAY * old_ref[0] + scale * total


def blend_layer(old_mats, terms, layer, inv_rows, written=None):
    dim = old_mats.shape[1]
    stacked = pl.BlockSpec((1, BLEND_ROWS, dim), lambda row: (layer, row, 0))
    plain = pl.BlockSpec((BLEND_ROWS, dim), lambda row: (row, 0))
    operands = [old_mats, *terms]
    in_specs = [stacked] + [plain] * len(terms)
    aliases = {}
    if written is not None:
        aliases = {len(operands): 0}
        operands.append(written)
        in_specs.append(pl.BlockSpec(memory_space=pl.ANY))
    return pl.pallas_call(
        functools.partial(blend_kernel, len(terms), (1.0 - FACTOR_DECAY) * inv_rows),
        out_shape=jax.ShapeDtypeStruct(old_mats.shape, jnp.float32),
        grid=(dim // BLEND_ROWS,),
        in_specs=in_specs,
        out_specs=stacked,
        input_output_aliases=aliases,
        cost_estimate=pl.CostEstimate(flops=10 ** 10, bytes_accessed=4 * dim * dim * (2 + len(terms)), transcendentals=0),
        compiler_params=pltpu.CompilerParams(vmem_limit_bytes=40 * 2 ** 20),
        name="blend_layer",
    )(*operands)


def solution(mesh):
    data_ways = mesh.shape['data']
    model_ways = mesh.shape['model']

    def to_rows(col_part):
        return lax.all_to_all(col_part, 'model', split_axis=0, concat_axis=1, tiled=True)

    def gather_weight(part):
        return lax.all_gather(core_half(part, 0, 0), ('model', 'data'), axis=0, tiled=True)

    def core_half(full, axis, shift):
        half = full.shape[axis] // data_ways
        core = (lax.axis_index('data') + shift) % data_ways
        return lax.dynamic_slice_in_dim(full, core * half, half, axis)

    def swap_cores(part):
        return lax.ppermute(part, 'data', SWAP)

    def pair_scatter(full, axis):
        return core_half(full, axis, 0) + swap_cores(core_half(full, axis, 1))

    def pair_gather(part, axis):
        other = swap_cores(part)
        return jnp.where(lax.axis_index('data') == 0, jnp.concatenate([part, other], axis), jnp.concatenate([other, part], axis))

    def own_gram(acts):
        width = acts.shape[1] // model_ways
        return matmul_tn(lax.dynamic_slice_in_dim(acts, lax.axis_index('model') * width, width, 1), acts)

    def whole_gram(part):
        part = lax.psum_scatter(part, 'data', scatter_dimension=0, tiled=True)
        return lax.all_gather(part, ('model', 'data'), axis=0, tiled=True)

    def layer_half(mats, layer, axis):
        half = mats.shape[axis] // data_ways
        starts = [layer, 0, 0]
        sizes = [1, mats.shape[1], mats.shape[2]]
        starts[axis] = lax.axis_index('data') * half
        sizes[axis] = half
        return lax.dynamic_slice(mats, starts, sizes).reshape(sizes[1:])

    def shard_body(x_tokens, dy_tokens, w_col, w_row, a_old_col, s_old_col, a_old_row, s_old_row, a_inv_col, s_inv_col, a_inv_row, s_inv_row):
        inv_rows = 1.0 / (x_tokens.shape[0] * data_ways)
        w_two = gather_weight(w_row[0])
        w_three_t = gather_weight(w_col[1].T)
        z_one = matmul(x_tokens, w_col[0]).astype(jnp.bfloat16)
        h_one = activate(z_one)
        h_one_t = to_rows(h_one)
        dh_three = matmul_nt(dy_tokens, w_row[1]).astype(jnp.bfloat16)
        a_one = matmul_tn(x_tokens, x_tokens)
        h_one_t, dh_three, a_one = lax.optimization_barrier((h_one_t, dh_three, a_one))
        dh_three_t = to_rows(dh_three)
        a_one_pair = swap_cores(a_one)
        z_two_t = matmul(h_one_t, w_two).astype(jnp.bfloat16)
        h_two_t = activate(z_two_t)
        h_two = lax.all_gather(h_two_t, 'model', axis=0, tiled=True)
        s_four = matmul_tn(dy_tokens, dy_tokens)
        a_one_rows = layer_half(a_inv_col, 0, 1)
        a_three_rows = layer_half(a_inv_col, 1, 1)
        s_two_cols = layer_half(s_inv_row, 0, 2)
        s_four_cols = layer_half(s_inv_row, 1, 2)
        (dh_three_t, s_four, a_one_rows, a_three_rows, s_two_cols, s_four_cols) = lax.optimization_barrier(
            (dh_three_t, s_four, a_one_rows, a_three_rows, s_two_cols, s_four_cols))
        s_four_pair = swap_cores(s_four)
        a_two = matmul_tn(h_one, h_one)
        z_three_t = matmul_nt(h_two_t, w_three_t).astype(jnp.bfloat16)
        g_three_t = back_gate(dh_three_t, z_three_t)
        dh_two_t = matmul(g_three_t, w_three_t).astype(jnp.bfloat16)
        g_two_t = back_gate(dh_two_t, z_two_t)
        g_two = lax.all_gather(g_two_t, 'model', axis=0, tiled=True)
        a_new_part = blend_layer(a_old_col, [a_one, a_one_pair], 0, inv_rows)
        s_new_part = blend_layer(s_old_row, [s_four, s_four_pair], 1, inv_rows)
        h_two, a_two, g_two_t, a_new_part, s_new_part = lax.optimization_barrier(
            (h_two, a_two, g_two_t, a_new_part, s_new_part))

        z_three = matmul(h_two, w_col[1]).astype(jnp.bfloat16)
        h_three = activate(z_three)
        g_three = back_gate(dh_three, z_three)
        grad_four = pair_scatter(matmul_tn(h_three, dy_tokens), 1) * inv_rows
        grad_three = pair_scatter(matmul_tn(h_two, g_three), 0) * inv_rows
        a_three = own_gram(h_two)
        a_four = matmul_tn(h_three, h_three)
        s_three = matmul_tn(g_three, g_three)
        left_four = pair_gather(exact_dot(a_inv_row[1], grad_four), 1)
        right_three = pair_gather(exact_dot(grad_three, s_inv_col[1]), 0)
        g_two, left_four, right_three, a_two, a_three, a_four, s_three = lax.optimization_barrier(
            (g_two, left_four, right_three, a_two, a_three, a_four, s_three))

        g_one = back_gate(matmul_nt(g_two, w_row[0]).astype(jnp.bfloat16), z_one)
        grad_one = lax.psum_scatter(matmul_tn(x_tokens, g_one), 'data', scatter_dimension=0, tiled=True) * inv_rows
        grad_two = lax.psum_scatter(matmul_tn(h_one, g_two), 'data', scatter_dimension=1, tiled=True) * inv_rows
        s_two = own_gram(g_two)
        s_one = matmul_tn(g_one, g_one)
        right_one = lax.all_gather(exact_dot(grad_one, s_inv_col[0]), 'data', axis=0, tiled=True)
        left_two = lax.all_gather(exact_dot(a_inv_row[0], grad_two), 'data', axis=1, tiled=True)
        right_one, left_two, a_three, s_two = lax.optimization_barrier((right_one, left_two, a_three, s_two))
        a_three = whole_gram(a_three)
        s_two = whole_gram(s_two)

        u_three = pair_gather(exact_dot(a_three_rows, right_three), 0)
        u_four = pair_gather(exact_dot(left_four, s_four_cols), 1)
        u_one = pair_gather(exact_dot(a_one_rows, right_one), 0)
        u_two = pair_gather(exact_dot(left_two, s_two_cols), 1)
        u_col = jnp.stack([u_one, u_three])
        u_row = jnp.stack([u_two, u_four])
        s_new_col = blend_blocks(s_old_col, (s_one, swap_cores(s_one)), (s_three, swap_cores(s_three)), inv_rows)
        a_new_row = blend_blocks(a_old_row, (a_two, swap_cores(a_two)), (a_four, swap_cores(a_four)), inv_rows)
        a_new_col = blend_layer(a_old_col, [a_three], 1, inv_rows, a_new_part)
        s_new_row = blend_layer(s_old_row, [s_two], 0, inv_rows, s_new_part)
        return (u_col, u_row, a_new_col, s_new_col, a_new_row, s_new_row)

    batch_split = P('data', None)
    col_split = P(None, None, 'model')
    row_split = P(None, 'model', None)
    replicated = P()
    return jax.shard_map(
        shard_body,
        mesh=mesh,
        in_specs=(batch_split, batch_split, col_split, row_split, replicated, row_split, row_split, replicated, replicated, row_split, row_split, replicated),
        out_specs=(col_split, row_split, replicated, row_split, row_split, replicated),
        check_vma=False,
    )
```
